32 devices in a mesh: rep: 4 (over x, y), dp: 8 (over z, core).
Axes of the slice: x: 2, y: 2, z: 4, core: 2. Of those that a mesh axis runs over, the one named last changes fastest.
Arguments:
- x: bfloat16 [32, 2048, 768], P(('rep', 'dp')), parts along dimension 0
- dy: bfloat16 [32, 2048, 768], P(('rep', 'dp')), parts along dimension 0
- wq: bfloat16 [2, 768, 768], P(None, 'dp')
- wk: bfloat16 [2, 768, 768], P(None, 'dp')
- wv: bfloat16 [2, 768, 768], P(None, 'dp')
- wo: bfloat16 [2, 768, 768], P(None, 'dp')
- w_gate: bfloat16 [2, 768, 3072], P(None, 'dp')
- w_up: bfloat16 [2, 768, 3072], P(None, 'dp')
- w_down: bfloat16 [2, 3072, 768], P(None, 'dp')
Outputs:
- output 1: bfloat16 [32, 2048, 768], P(('rep', 'dp')), parts along dimension 0
- output 2: bfloat16 [8, 768, 768], P('rep', 'dp'), parts along dimension 0
- output 3: bfloat16 [8, 768, 768], P('rep', 'dp'), parts along dimension 0
- output 4: bfloat16 [8, 768, 768], P('rep', 'dp'), parts along dimension 0
- output 5: bfloat16 [8, 768, 768], P('rep', 'dp'), parts along dimension 0
- output 6: bfloat16 [8, 768, 3072], P('rep', 'dp'), parts along dimension 0
- output 7: bfloat16 [8, 768, 3072], P('rep', 'dp'), parts along dimension 0
- output 8: bfloat16 [8, 3072, 768], P('rep', 'dp'), parts along dimension 0
There are 4 independent parts. The reference program is written for one: setup_inputs(seed, part) draws one part's arguments, and reference() takes and returns one part's arrays. A program takes and returns all parts, laid end to end along the dimension named above; an argument that names none is the same for every part.
All inputs are finite; a program needn't handle non-finite values.
Results may differ from the reference program's by a relative error of at most 0.0327.
Values are sent between devices in bfloat16 or wider.
A program may use at most 2 GiB of HBM per device.

```python
import jax
import jax.numpy as jnp
from jax import lax

SEQUENCES = 8
TOKENS = 2048
D = 768
HEADS = 6
KV_HEADS = 6
HEAD = 128
FF = 3072
LAYERS = 2
THETA = 10000
NAMES = ("wq", "wk", "wv", "wo", "w_gate", "w_up", "w_down")
SHAPES = {
    "wq": (LAYERS, D, HEADS * HEAD),
    "wk": (LAYERS, D, KV_HEADS * HEAD),
    "wv": (LAYERS, D, KV_HEADS * HEAD),
    "wo": (LAYERS, HEADS * HEAD, D),
    "w_gate": (LAYERS, D, FF),
    "w_up": (LAYERS, D, FF),
    "w_down": (LAYERS, FF, D),
}


def bump(key, n, height):
    away = (jnp.arange(n, dtype=jnp.int32) - jax.random.randint(key, (), 0, n, jnp.int32)) % n
    return jnp.where(away < n // 8, height, 1.0)


def together(key, own, strength):
    shared = jax.random.normal(key, own.shape[1:], jnp.float32)
    return (own + strength * shared) * lax.rsqrt(1 + strength * strength)


def setup_inputs(seed: int = 0, part: int = 0) -> dict:
    kx, kdy, ka, kb, kz, kf, kh, kl, *keys = jax.random.split(jax.random.key(seed), 8 + 3 * len(NAMES))
    kx, kdy, ka, kb = (jax.random.fold_in(k, part) for k in (kx, kdy, ka, kb))
    kw, km, kv = (keys[i::3] for i in range(3))
    shape = (SEQUENCES, TOKENS, D)
    much_x, much_dy = jax.random.uniform(kz, (2,), jnp.float32, 0.0, 1.0)
    loud = 2.0 ** jax.random.uniform(jax.random.fold_in(kz, 1), (), jnp.float32, -1.0, 2.0)
    layers = 2.0 ** jax.random.uniform(kl, (LAYERS, 1, 1), jnp.float32, -1.0, 1.0)
    times = {"wq": 1.0, "wk": 1.0, "wv": 2.0, "wo": layers, "w_gate": 1.0, "w_up": bump(kh, FF, 4.0), "w_down": layers}
    x = together(ka, jax.random.normal(kx, shape, jnp.float32), much_x) * bump(kf, D, 4.0)
    dy = together(kb, jax.random.normal(kdy, shape, jnp.float32), much_dy)
    drawn = {"x": x.astype(jnp.bfloat16), "dy": (loud * dy * (SEQUENCES * TOKENS) ** -0.5).astype(jnp.bfloat16)}
    for key, name in zip(kw, NAMES, strict=True):
        drawn[name] = (jax.random.normal(key, SHAPES[name], jnp.float32) * SHAPES[name][1] ** -0.5 * times[name]).astype(jnp.bfloat16)
    return drawn


def matmul(a, w):
    return jnp.dot(a, w, preferred_element_type=jnp.float32).astype(jnp.bfloat16)


def normed(h):
    wide = h.astype(jnp.float32)
    scale = lax.rsqrt(jnp.mean(wide**2, -1, keepdims=True) + 1e-6)
    return (wide * scale).astype(jnp.bfloat16)


def turned(t, theta):
    half = t.shape[-1] // 2
    angle = jnp.arange(t.shape[0], dtype=jnp.float32)[:, None] * theta ** (-jnp.arange(half, dtype=jnp.float32) / half)
    cos, sin = jnp.cos(angle)[:, None], jnp.sin(angle)[:, None]
    a, b = t[..., :half].astype(jnp.float32), t[..., half:].astype(jnp.float32)
    return jnp.concatenate([a * cos - b * sin, b * cos + a * sin], -1).astype(jnp.bfloat16)


def seen_by(q, k, v):
    tokens, kv = q.shape[0], k.shape[1]
    q = q.reshape(tokens, kv, -1, q.shape[-1])
    scores = jnp.einsum("tgsd,ugd->gstu", q.astype(jnp.float32), k.astype(jnp.float32)) * q.shape[-1] ** -0.5
    place = jnp.arange(tokens)
    weights = jax.nn.softmax(jnp.where(place[:, None] >= place, scores, -jnp.inf), -1).astype(jnp.bfloat16)
    return jnp.einsum("gstu,ugd->tgsd", weights.astype(jnp.float32), v.astype(jnp.float32)).astype(jnp.bfloat16).reshape(tokens, -1)


def layer(h, w):
    a = normed(h)
    q, k = (turned(matmul(a, w[name]).reshape(h.shape[0], -1, HEAD), THETA) for name in ("wq", "wk"))
    h = h + matmul(seen_by(q, k, matmul(a, w["wv"]).reshape(h.shape[0], -1, HEAD)), w["wo"])
    b = normed(h)
    gate = jnp.dot(b, w["w_gate"], preferred_element_type=jnp.float32)
    up = jnp.dot(b, w["w_up"], preferred_element_type=jnp.float32)
    return h + matmul((jax.nn.silu(gate) * up).astype(jnp.bfloat16), w["w_down"])


def stack(weights, h):
    return lax.scan(lambda h, w: (layer(h, w), None), h, weights)[0]


def reference(x, dy, wq, wk, wv, wo, w_gate, w_up, w_down):
    weights = dict(zip(NAMES, (wq, wk, wv, wo, w_gate, w_up, w_down), strict=True))

    def take(so_far, sequence):
        h, by_y = sequence
        _, back = jax.vjp(stack, weights, h)
        by_weights, by_h = back(by_y)
        return jax.tree.map(lambda total, term: total + term.astype(jnp.float32), so_far, by_weights), by_h

    none_yet = {name: jnp.zeros(w.shape, jnp.float32) for name, w in weights.items()}
    by_weights, by_x = lax.scan(take, none_yet, (x, dy))
    return (by_x, *(by_weights[name].astype(jnp.bfloat16) for name in NAMES))
```

```python
import functools

import jax
import jax.numpy as jnp
import numpy as np
from jax import lax
from jax.experimental import pallas as pl
from jax.experimental.pallas import tpu as pltpu
from jax.sharding import PartitionSpec as P

NEG = -1e30
HIDDEN = 2 * NEG
LOG2E = 1.4426950408889634
VMEM = 56 * 2**20
HEAD = 128
THETA = 10000
EPS = 1e-6
BT = 512
MESH = pl.DeviceIdType.MESH
bf16, f32 = jnp.bfloat16, jnp.float32


def _dot(a, b, ca, cb):
    return lax.dot_general(a, b, (((ca,), (cb,)), ((), ())), preferred_element_type=f32)


def _mm(a, b):
    return _dot(a, b, 1, 0)


def _mt(a, b):
    return _dot(a, b, 1, 1)


def _tm(a, b):
    return _dot(a, b, 0, 0)


def _params(*semantics):
    return pltpu.CompilerParams(dimension_semantics=semantics, vmem_limit_bytes=VMEM)


def _estimate(flops, *arrays):
    return pl.CostEstimate(flops=int(flops), transcendentals=0, bytes_accessed=sum(a.size * a.dtype.itemsize for a in arrays))


def _like(*shape, dtype=bf16):
    return jax.ShapeDtypeStruct(shape, dtype)


def _visible(keys, wide, at):
    return lax.broadcasted_iota(jnp.int32, (keys, wide), 0) <= lax.broadcasted_iota(jnp.int32, (keys, wide), 1) + at


def _strips(size, cut):
    half = size // 2
    return [(0, half, half), (half, half, size)] if cut else [(0, size, size)]


def _over_blocks(block):
    iq = pl.program_id(1)
    lax.fori_loop(0, iq, lambda j, _: block(pl.multiple_of(j * BT, BT), False), None)
    block(pl.multiple_of(iq * BT, BT), True)


def _attend(q_ref, k_ref, v_ref, o_ref, lse_ref, top_s, mix_s):
    heads, size, d = q_ref.shape
    scale = d**-0.5
    e = scale * LOG2E
    top_s[...] = jnp.full(top_s.shape, NEG, f32)
    mix_s[...] = jnp.zeros(mix_s.shape, f32)

    def block(start, diagonal):
        pieces = [(i, *strip) for i in range(heads) for strip in _strips(size, diagonal)]
        scores = [_mt(k_ref[i, pl.ds(start, keys), :], q_ref[i, at : at + wide, :]) for i, at, wide, keys in pieces]
        weights, keeps = [], []
        for (i, at, wide, keys), s in zip(pieces, scores):
            if diagonal:
                s = jnp.where(_visible(keys, wide, at), s, HIDDEN)
            old = top_s[i : i + 1, at : at + wide]
            top = jnp.maximum(old, s.max(axis=0, keepdims=True))
            top_s[i : i + 1, at : at + wide] = top
            weights.append(jnp.exp2((s - top) * e).astype(bf16))
            keeps.append(jnp.exp2((old - top) * e))
        for (i, at, wide, keys), p, keep in zip(pieces, weights, keeps):
            values = jnp.concatenate([v_ref[i, pl.ds(start, keys), :].T, jnp.ones((8, keys), bf16)], axis=0)
            mix_s[i, :, at : at + wide] = mix_s[i, :, at : at + wide] * keep + _mm(values, p)

    _over_blocks(block)
    for i in range(heads):
        total = mix_s[i, d : d + 1, :]
        o_ref[i] = (mix_s[i, :d, :] * (1 / total)).T.astype(bf16)
        lse_ref[i : i + 1, :] = top_s[i : i + 1, :] * scale + jnp.log(total)


def attend(q, k, v):
    n, t, d = q.shape
    block = pl.BlockSpec((n, BT, d), lambda h, i: (h, i, 0))
    whole = pl.BlockSpec((n, t, d), lambda h, i: (h, 0, 0))
    return pl.pallas_call(
        _attend, grid=(1, t // BT), in_specs=[block, whole, whole], out_specs=[block, pl.BlockSpec((n, BT), lambda h, i: (h, i))],
        out_shape=[_like(n, t, d), _like(n, t, dtype=f32)], scratch_shapes=[pltpu.VMEM((n, BT), f32), pltpu.VMEM((n, d + 8, BT), f32)],
        compiler_params=_params("parallel", "arbitrary"), cost_estimate=_estimate(4 * n * t * t * d, q, q, k, v), name="attend",
    )(q, k, v)


def _attend_back(q_ref, k_ref, v_ref, do_ref, lse_ref, delta_ref, dq_ref, dk_ref, dv_ref, dq_s, dk_s, dv_s):
    heads, size, d = q_ref.shape
    iq = pl.program_id(1)
    scale = d**-0.5
    e = scale * LOG2E

    @pl.when(iq == 0)
    def _():
        dk_s[...] = jnp.zeros(dk_s.shape, f32)
        dv_s[...] = jnp.zeros(dv_s.shape, f32)

    dq_s[...] = jnp.zeros(dq_s.shape, f32)

    def block(start, diagonal):
        pieces = [(i, *strip) for i in range(heads) for strip in _strips(size, diagonal)]
        rows = [pl.ds(start, keys) for _, _, _, keys in pieces]
        qs = [q_ref[i, at : at + wide, :] for i, at, wide, _ in pieces]
        dos = [do_ref[i, at : at + wide, :] for i, at, wide, _ in pieces]
        scores = [_mt(k_ref[piece[0], here, :], x) for piece, here, x in zip(pieces, rows, qs)]
        dps = [_mt(v_ref[piece[0], here, :], x) for piece, here, x in zip(pieces, rows, dos)]
        for (i, at, wide, keys), here, s, dp, q, do in zip(pieces, rows, scores, dps, qs, dos):
            p = jnp.exp2(s * e - lse_ref[0, i : i + 1, at : at + wide] * LOG2E)
            if diagonal:
                p = jnp.where(_visible(keys, wide, at), p, 0)
            ds = (p * (dp - delta_ref[0, i : i + 1, at : at + wide])).astype(bf16)
            dv_s[i, here, :] += _mm(p.astype(bf16), do)
            dk_s[i, here, :] += _mm(ds, q)
            dq_s[i, :, at : at + wide] += _mm(k_ref[i, here, :].T, ds)

    _over_blocks(block)
    for i in range(heads):
        dq_ref[i] = (dq_s[i] * scale).T.astype(bf16)

    @pl.when(iq == pl.num_programs(1) - 1)
    def _():
        dk_ref[...] = (dk_s[...] * scale).astype(bf16)
        dv_ref[...] = dv_s[...].astype(bf16)


def attend_back(q, k, v, do, lse, delta):
    n, t, d = q.shape
    some = n // 2
    block = pl.BlockSpec((some, BT, d), lambda h, i: (h, i, 0))
    whole = pl.BlockSpec((some, t, d), lambda h, i: (h, 0, 0))
    stats = pl.BlockSpec((1, some, BT), lambda h, i: (h, 0, i))
    return pl.pallas_call(
        _attend_back, grid=(n // some, t // BT), in_specs=[block, whole, whole, block, stats, stats], out_specs=[block, whole, whole],
        out_shape=[_like(n, t, d)] * 3,
        scratch_shapes=[pltpu.VMEM((some, d, BT), f32)] + [pltpu.VMEM((some, t, d), f32)] * 2,
        compiler_params=_params("parallel", "arbitrary"), cost_estimate=_estimate(10 * n * t * t * d, q, q, k, k, v, v, do), name="attend_back",
    )(q, k, v, do, lse.reshape(-1, some, t), delta.reshape(-1, some, t))


def _once(w):
    return pl.BlockSpec((w[0].shape[0], w[1]), lambda *_: (0, w[2]), pipeline_mode=pl.Buffered(1))


def _bring(s, weights, sems):
    def copies(t):
        for n, (src, place, dst, axis) in enumerate(weights):
            size = dst.shape[axis] // 2
            cut = pl.ds(t * size, size)
            if axis:
                pair = src.at[:, pl.ds(place * dst.shape[1] + t * size, size)], dst.at[:, cut]
            else:
                pair = src.at[cut, pl.ds(place * dst.shape[1], dst.shape[1])], dst.at[cut]
            yield pltpu.make_async_copy(*pair, sems.at[t, n])

    @pl.when(s == 0)
    def _():
        for copy in (*copies(0), *copies(1)):
            copy.start()

    def wait():
        for t in range(2):

            @pl.when(s == t)
            def _(t=t):
                for copy in copies(t):
                    copy.wait()

    return wait


def _room(*weights):
    return [pltpu.VMEM((w[0].shape[0], w[1]), bf16) for w in weights] + [pltpu.SemaphoreType.DMA((2, len(weights)))]


def _norm(h):
    scale = lax.rsqrt(jnp.mean(h * h, -1, keepdims=True) + EPS)
    return h * scale, scale


def _norm_back(by, h, scale):
    inner = jnp.mean(by * h, -1, keepdims=True)
    return scale * by - h * (scale * scale * scale * inner)


def _sigmoid(g):
    return 0.5 * jnp.tanh(0.5 * g) + 0.5


def _heads(ref):
    return jnp.concatenate([ref[i] for i in range(ref.shape[0])], axis=1)


def table(tokens):
    half = HEAD // 2
    angle = np.arange(tokens, dtype=np.float32)[:, None] * np.float32(THETA) ** (-np.arange(half, dtype=np.float32) / half)
    return jnp.asarray(np.concatenate([np.cos(angle), np.sin(angle)], 1), f32)


def _spread(turn_ref):
    both = turn_ref[...]
    swapped = pltpu.roll(both, HEAD // 2, 1)
    low = lax.broadcasted_iota(jnp.int32, both.shape, 1) < HEAD // 2
    return jnp.where(low, both, swapped), jnp.where(low, -swapped, both)


def _qkv(h_ref, turn_ref, wq_ref, wk_ref, wv_ref, a_ref, q_ref, k_ref, v_ref):
    a = _norm(h_ref[...].astype(f32))[0].astype(bf16)
    a_ref[...] = a
    cos, sin = _spread(turn_ref)
    for w_ref, out in ((wq_ref, q_ref), (wk_ref, k_ref), (wv_ref, v_ref)):
        t = _mm(a, w_ref[...]).astype(bf16)
        for i in range(out.shape[0]):
            one = t[:, i * HEAD : (i + 1) * HEAD]
            if out is not v_ref:
                wide = one.astype(f32)
                one = (wide * cos + pltpu.roll(wide, HEAD // 2, 1) * sin).astype(bf16)
            out[i] = one


def qkv(h, turn, wq, wk, wv):
    t, d = h.shape
    n = wq[1] // HEAD
    row, tab = pl.BlockSpec((BT, d), lambda i: (i, 0)), pl.BlockSpec((BT, HEAD), lambda i: (i, 0))
    heads = pl.BlockSpec((n, BT, HEAD), lambda i: (0, i, 0))
    shape = _like(n, t, HEAD)
    return pl.pallas_call(
        _qkv, grid=(t // BT,), in_specs=[row, tab] + [_once(w) for w in (wq, wk, wv)], out_specs=[row] + [heads] * 3,
        out_shape=[_like(*h.shape)] + [shape] * 3, compiler_params=_params("arbitrary"),
        cost_estimate=_estimate(6 * t * d * d, h, h, h, h, h, h), name="qkv",
    )(h, turn, wq[0], wk[0], wv[0])


CH = 768


def _hidden(b, wg_ref, wu_ref, here):
    return _mm(b, wg_ref[:, here]), _mm(b, wu_ref[:, here])


def _chunks(s):
    j = lax.rem(s, 2)
    return [pl.ds(pl.multiple_of(n * CH, CH), CH) for n in (2 * j, 2 * j + 1, jnp.where(s == 0, 1, lax.rem(2 * j + 3, 4)))]


def _enter(h_ref, o_ref, wo_ref, h1_ref, b_ref, b_s):
    h1 = (h_ref[...].astype(f32) + _mm(_heads(o_ref), wo_ref[...]).astype(bf16).astype(f32)).astype(bf16)
    h1_ref[...] = h1
    b = _norm(h1.astype(f32))[0].astype(bf16)
    b_ref[...] = b
    b_s[...] = b
    return h1


def _ffn(h_ref, o_ref, wo_ref, wg_in, wu_in, wd_in, h1_ref, b_ref, g_ref, u_ref, act_ref, h2_ref, acc_s, all_s, act_s, b_s, h1_s, old_s,
         wg_ref, wu_ref, wd_ref, sems, *, places):
    s, last = pl.program_id(0), pl.num_programs(0) - 1
    j = lax.rem(s, 2)
    first, second, before = _chunks(s)
    brought = _bring(s, [(wg_in, places[0], wg_ref, 1), (wu_in, places[1], wu_ref, 1), (wd_in, places[2], wd_ref, 0)], sems)

    @pl.when((j == 0) & (s < last))
    def _():
        old_s[...] = h1_s[...]
        h1_s[...] = _enter(h_ref, o_ref, wo_ref, h1_ref, b_ref, b_s)

    brought()

    @pl.when(s < last)
    def _():
        b = b_s[...]
        g, u = _hidden(b, wg_ref, wu_ref, first)
        left = _mm(act_s[...], wd_ref[before, :])
        g_ref[:, :CH] = g
        u_ref[:, :CH] = u
        one = (g * _sigmoid(g) * u).astype(bf16)
        act_ref[:, :CH] = one
        g, u = _hidden(b, wg_ref, wu_ref, second)
        right = _mm(one, wd_ref[first, :])
        g_ref[:, CH:] = g
        u_ref[:, CH:] = u
        two = (g * _sigmoid(g) * u).astype(bf16)
        act_ref[:, CH:] = two
        act_s[...] = two
        total = acc_s[...] + left
        all_s[...] = total
        acc_s[...] = right + jnp.where(j == 0, 0.0, total)

    @pl.when(s == last)
    def _():
        all_s[...] = acc_s[...] + _mm(act_s[...], wd_ref[before, :])
        old_s[...] = h1_s[...]

    @pl.when((j == 0) & (s > 0))
    def _():
        h2_ref[...] = (old_s[...].astype(f32) + all_s[...].astype(bf16).astype(f32)).astype(bf16)


def _act(h_ref, o_ref, wo_ref, wg_in, wu_in, h1_ref, b_ref, g_ref, u_ref, act_ref, b_s, wg_ref, wu_ref, sems, *, places):
    s = pl.program_id(0)
    j = lax.rem(s, 2)
    brought = _bring(s, [(wg_in, places[0], wg_ref, 1), (wu_in, places[1], wu_ref, 1)], sems)

    @pl.when(j == 0)
    def _():
        _enter(h_ref, o_ref, wo_ref, h1_ref, b_ref, b_s)

    brought()
    for p, here in enumerate(_chunks(s)[:2]):
        g, u = _hidden(b_s[...], wg_ref, wu_ref, here)
        columns = pl.ds(p * CH, CH)
        g_ref[:, columns] = g
        u_ref[:, columns] = u
        act_ref[:, columns] = (g * _sigmoid(g) * u).astype(bf16)


def _blocks(t, d, n):
    steps = t // BT * 2
    now, was = lambda s: jnp.minimum(s, steps - 1), lambda s: jnp.maximum(s - 1, 0)
    row = lambda at: pl.BlockSpec((BT, d), lambda s: (at(s) // 2, 0))
    heads = lambda at: pl.BlockSpec((n, BT, HEAD), lambda s: (0, at(s) // 2, 0))
    return steps, row(now), row(was), pl.BlockSpec((BT, 2 * CH), lambda s: (now(s) // 2, now(s) % 2)), heads(now), heads(was)


def ffn(h, o, wo, wg, wu, wd=None):
    t, d = h.shape
    ff = wg[1]
    steps, row, late, wide, heads, late_heads = _blocks(t, d, o.shape[0])
    same = _like(*h.shape)
    hidden, product = _like(t, ff, dtype=f32), _like(t, ff)
    down = wd is not None
    given = [wg, wu] + [wd] * down
    state = [pltpu.VMEM((BT, d), f32)] * 2 + [pltpu.VMEM((BT, CH), bf16)]
    return pl.pallas_call(
        functools.partial(_ffn if down else _act, places=[w[2] for w in given]), grid=(steps + down,),
        in_specs=[row, heads, _once(wo)] + [pl.BlockSpec(memory_space=pltpu.HBM)] * len(given),
        out_specs=[row, row, wide, wide, wide] + [late] * down, out_shape=[same, same, hidden, hidden, product] + [same] * down,
        scratch_shapes=(state if down else []) + [pltpu.VMEM((BT, d), bf16)] * (3 if down else 1) + _room(*given),
        compiler_params=_params("arbitrary"),
        cost_estimate=_estimate(2 * t * d * (d + (3 if down else 2) * ff), h, h, h, h, *(w[0] for w in given), hidden, hidden, product), name="ffn",
    )(h, o, wo[0], *(w[0] for w in given))


def _ffn_back(h1_ref, dh_ref, late_ref, o_ref, g_ref, u_ref, wo_ref, wd_in, wg_in, wu_in, dg_ref, du_ref, dh1_ref, do_ref, delta_ref,
              acc_s, all_s, dg_s, du_s, wd_ref, wg_ref, wu_ref, sems, *, places):
    s, last = pl.program_id(0), pl.num_programs(0) - 1
    j = lax.rem(s, 2)
    first, second, before = _chunks(s)

    def back(dg, du, here):
        return _mt(dg, wg_ref[:, here]) + _mt(du, wu_ref[:, here])

    def through(by, p):
        columns = pl.ds(p * CH, CH)
        g, u = g_ref[:, columns], u_ref[:, columns]
        by = by.astype(bf16).astype(f32)
        gate = _sigmoid(g)
        silu = g * gate
        dg = (by * u * (gate + silu * (1 - gate))).astype(bf16)
        du = (by * silu).astype(bf16)
        dg_ref[:, columns] = dg
        du_ref[:, columns] = du
        return dg, du

    _bring(s, [(wd_in, places[0], wd_ref, 0), (wg_in, places[1], wg_ref, 1), (wu_in, places[2], wu_ref, 1)], sems)()

    @pl.when(s < last)
    def _():
        dh = dh_ref[...]
        one = through(_mt(dh, wd_ref[first, :]), 0)
        left = back(dg_s[...], du_s[...], before)
        two = through(_mt(dh, wd_ref[second, :]), 1)
        right = back(*one, first)
        dg_s[...], du_s[...] = two
        total = acc_s[...] + left
        all_s[...] = total
        acc_s[...] = right + jnp.where(j == 0, 0.0, total)

    @pl.when(s == last)
    def _():
        all_s[...] = acc_s[...] + back(dg_s[...], du_s[...], before)

    @pl.when((j == 0) & (s > 0))
    def _():
        h1 = h1_ref[...].astype(f32)
        slope = _norm_back(all_s[...].astype(bf16).astype(f32), h1, _norm(h1)[1])
        dh1 = (late_ref[...].astype(f32) + slope.astype(bf16).astype(f32)).astype(bf16)
        dh1_ref[...] = dh1
        do = _mt(dh1, wo_ref[...]).astype(bf16)
        n = o_ref.shape[0]
        for i in range(n):
            do_ref[i] = do[:, i * HEAD : (i + 1) * HEAD]
        width = n * HEAD
        ones = (lax.broadcasted_iota(jnp.int32, (8, width), 1) // HEAD == lax.broadcasted_iota(jnp.int32, (8, width), 0)).astype(bf16)
        left = do.astype(f32) * _heads(o_ref).astype(f32)
        pieces = []
        for _ in range(3):
            pieces.append(left.astype(bf16))
            left = left - pieces[-1].astype(f32)
        delta_ref[...] = sum(_mt(ones, piece) for piece in pieces)[:n]


def ffn_back(h1, dh, o, gate, up, wo, wg, wu, wd):
    t, d = h1.shape
    ff, n = wg[1], o.shape[0]
    steps, row, late, wide, _, heads = _blocks(t, d, n)
    stats = pl.BlockSpec((n, BT), lambda s: heads.index_map(s)[:2])
    same = _like(*h1.shape)
    hidden = _like(t, ff)
    brought = [wd, wg, wu]
    given = [h1, dh, dh, o, gate, up, wo[0]] + [w[0] for w in brought]
    return pl.pallas_call(
        functools.partial(_ffn_back, places=[w[2] for w in brought]), grid=(steps + 1,),
        in_specs=[late, row, late, heads, wide, wide, _once(wo)] + [pl.BlockSpec(memory_space=pltpu.HBM)] * len(brought),
        out_specs=[wide, wide, late, heads, stats],
        out_shape=[hidden, hidden, same, _like(*o.shape), _like(n, t, dtype=f32)],
        scratch_shapes=[pltpu.VMEM((BT, d), f32)] * 2 + [pltpu.VMEM((BT, CH), bf16)] * 2 + _room(*brought),
        compiler_params=_params("arbitrary"), cost_estimate=_estimate(2 * t * d * (d + 3 * ff), *given, hidden, hidden, h1, h1), name="ffn_back",
    )(*given)


def _qkv_back(h_ref, dh1_ref, dq_ref, dk_ref, dv_ref, turn_ref, wq_ref, wk_ref, wv_ref, dh_ref, all_ref):
    cos, sin = _spread(turn_ref)
    n, d = dq_ref.shape[0], h_ref.shape[1]
    da = None
    for m, (ref, w_ref) in enumerate(((dq_ref, wq_ref), (dk_ref, wk_ref), (dv_ref, wv_ref))):
        for i in range(n):
            one = ref[i]
            if ref is not dv_ref:
                wide = one.astype(f32)
                one = (wide * cos - pltpu.roll(wide, HEAD // 2, 1) * sin).astype(bf16)
            all_ref[:, (m * n + i) * HEAD : (m * n + i + 1) * HEAD] = one
        part = _mt(all_ref[:, m * n * HEAD : (m + 1) * n * HEAD], w_ref[...])
        da = part if da is None else da + part
    h = h_ref[...].astype(f32)
    back = _norm_back(da.astype(bf16).astype(f32), h, _norm(h)[1])
    dh_ref[...] = (dh1_ref[...].astype(f32) + back.astype(bf16).astype(f32)).astype(bf16)


def qkv_back(h, dh1, dq, dk, dv, turn, wq, wk, wv):
    t, d = h.shape
    n = dq.shape[0]
    row, tab = pl.BlockSpec((BT, d), lambda i: (i, 0)), pl.BlockSpec((BT, HEAD), lambda i: (i, 0))
    heads = pl.BlockSpec((n, BT, HEAD), lambda i: (0, i, 0))
    return pl.pallas_call(
        _qkv_back, grid=(t // BT,), in_specs=[row, row, heads, heads, heads, tab] + [_once(w) for w in (wq, wk, wv)],
        out_specs=[row, pl.BlockSpec((BT, 3 * n * HEAD), lambda i: (i, 0))],
        out_shape=[_like(*h.shape), _like(t, 3 * n * HEAD)],
        compiler_params=_params("arbitrary"),
        cost_estimate=_estimate(6 * t * d * d, h, h, dq, dk, dv, h, h, h, h, h), name="qkv_back",
    )(h, dh1, dq, dk, dv, turn, wq[0], wk[0], wv[0])


def _weights(a_ref, b_ref, out_ref):
    out_ref[...] = _tm(a_ref[...], b_ref[...]).astype(bf16)


def by_weight(a, b, rows, cols):
    t, m = a.shape
    n = b.shape[1]
    return pl.pallas_call(
        _weights, grid=(m // rows, n // cols),
        in_specs=[pl.BlockSpec((t, rows), lambda i, j: (0, i)), pl.BlockSpec((t, cols), lambda i, j: (0, j))],
        out_specs=pl.BlockSpec((rows, cols), lambda i, j: (i, j)), out_shape=_like(m, n),
        compiler_params=_params("arbitrary", "arbitrary"), cost_estimate=_estimate(2 * t * m * n, a, b), name="by_weight",
    )(a, b)


def _weights_ffn(b_ref, dg_ref, du_ref, out_ref, *, parts):
    for ref, mine in ((dg_ref, pl.program_id(0) < parts), (du_ref, pl.program_id(0) >= parts)):

        @pl.when(mine)
        def _(ref=ref):
            out_ref[...] = _tm(b_ref[...], ref[...]).astype(bf16)


def by_ffn_weights(b, dg, du):
    (t, d), ff = b.shape, dg.shape[1]
    parts = ff // d
    tile = lambda first: pl.BlockSpec((t, d), lambda j: (0, jnp.clip(j - first, 0, parts - 1)))
    return pl.pallas_call(
        functools.partial(_weights_ffn, parts=parts), grid=(2 * parts,), in_specs=[_once((b, d, 0)), tile(0), tile(parts)],
        out_specs=pl.BlockSpec((d, d), lambda j: (0, j)), out_shape=_like(d, 2 * ff), compiler_params=_params("arbitrary"),
        cost_estimate=_estimate(4 * t * d * ff, b, b, dg, du), name="by_ffn_weights",
    )(b, dg, du)


def _weights_attention(a_ref, dqkv_ref, o_ref, dh1_ref, out_ref):
    j, last = pl.program_id(0), pl.num_programs(0) - 1

    @pl.when(j < last)
    def _():
        out_ref[...] = _tm(a_ref[...], dqkv_ref[...]).astype(bf16)

    @pl.when(j == last)
    def _():
        for i in range(o_ref.shape[0]):
            out_ref[i * HEAD : (i + 1) * HEAD, :] = _tm(o_ref[i], dh1_ref[...]).astype(bf16)


def by_attention_weights(a, dqkv, o, dh1):
    t, d = a.shape
    parts = dqkv.shape[1] // d
    whole = pl.BlockSpec(o.shape, lambda j: (0, 0, 0), pipeline_mode=pl.Buffered(1))
    return pl.pallas_call(
        _weights_attention, grid=(parts + 1,),
        in_specs=[_once((a, d, 0)), pl.BlockSpec((t, d), lambda j: (0, jnp.minimum(j, parts - 1))), whole, _once((dh1, d, 0))],
        out_specs=pl.BlockSpec((d, d), lambda j: (0, j)), out_shape=_like(d, (parts + 1) * d), compiler_params=_params("arbitrary"),
        cost_estimate=_estimate(2 * t * d * d * (parts + 1), a, dqkv, o, dh1), name="by_attention_weights",
    )(a, dqkv, o, dh1)


def _gather(*refs, n, number):
    own, out, vm = refs[:n], refs[n : 2 * n], refs[2 * n : 3 * n]
    us, ds, zr, xs, xr, ys, yr, fs, fr, cs, cr, lin, lout = refs[3 * n :]
    rep, dp = lax.axis_index("rep"), lax.axis_index("dp")
    z, c = lax.div(dp, 2), lax.rem(dp, 2)
    flipped = lambda group: group + 1 - 2 * lax.rem(group, 2)
    beside_x, beside_y = lax.rem(rep + 2, 4), flipped(rep)
    across = flipped(beside_x)
    others = [lax.rem(z + jnp.where(z < 2, k, 4 - k), 4) for k in (1, 3, 2)]
    partner = (rep, 2 * z + 1 - c)

    barrier = pltpu.get_barrier_semaphore()
    for peer in [(rep, 2 * o + c) for o in others] + [(beside_x, dp), (beside_y, dp), partner]:
        pl.semaphore_signal(barrier, inc=1, device_id=peer, device_id_type=MESH)
    pl.semaphore_wait(barrier, 6)

    sizes = [w.shape[1] // 4 for w in own]

    def slice_of(m, zz, group):
        return out[m].at[pl.ds(pl.multiple_of((8 * zz + 4 * c + group) * sizes[m], sizes[m]), sizes[m])]

    def shard_of(m, zz, cc):
        return out[m].at[pl.ds(pl.multiple_of((8 * zz + 4 * cc) * sizes[m], 4 * sizes[m]), 4 * sizes[m])]

    def send(src, dst, send_sem, recv_sem, peer):
        return pltpu.make_async_remote_copy(src_ref=src, dst_ref=dst, send_sem=send_sem, recv_sem=recv_sem, device_id=peer, device_id_type=MESH)

    def mine(m):
        return own[m].at[number, pl.ds(pl.multiple_of(rep * sizes[m], sizes[m]), sizes[m])]

    def up(m, o):
        src = mine(m) if o is z else slice_of(m, o, rep)
        return send(src, slice_of(m, o, rep), us.at[m, o], zr.at[m, o], (rep, jnp.minimum(2 * z + 2, 6) + c))

    def down(m, o):
        src = mine(m) if o is z else slice_of(m, o, rep)
        return send(src, slice_of(m, o, rep), ds.at[m, o], zr.at[m, o], (rep, jnp.maximum(2 * z - 2, 0) + c))

    def further(m, o, act):
        @pl.when((o <= z) & (z < 3))
        def _():
            act(up(m, o))

        @pl.when((o >= z) & (z > 0))
        def _():
            act(down(m, o))

    def from_z(m, o):
        return send(mine(m), slice_of(m, o, rep), us.at[m, 0], zr.at[m, o], (rep, 2 * o + c))

    def to_x(m, k, o):
        return send(slice_of(m, o, rep), slice_of(m, o, rep), xs.at[m, k], xr.at[m, o], (beside_x, dp))

    def to_y(m, k, o):
        return send(slice_of(m, o, rep), slice_of(m, o, rep), ys.at[m, k], yr.at[m, o], (beside_y, dp))

    def from_x(m, o):
        return send(slice_of(m, o, beside_x), slice_of(m, o, beside_x), xs.at[m, 0], xr.at[m, o], (beside_x, dp))

    def from_y(m, o):
        return send(slice_of(m, o, beside_y), slice_of(m, o, beside_y), ys.at[m, 0], yr.at[m, o], (beside_y, dp))

    def onward(m, k, o):
        if (m + k) % 2:
            return send(slice_of(m, o, beside_y), slice_of(m, o, beside_y), fs.at[m, k], fr.at[m, k], (beside_x, dp))
        return send(slice_of(m, o, beside_x), slice_of(m, o, beside_x), fs.at[m, k], fr.at[m, k], (beside_y, dp))

    def from_onward(m, k, o):
        return send(slice_of(m, o, across), slice_of(m, o, across), fs.at[m, k], fr.at[m, k], (beside_x, dp))

    def to_core(m, k):
        zz = z if k == 3 else others[k]
        src = own[m].at[number] if k == 3 else shard_of(m, zz, c)
        return send(src, shard_of(m, zz, c), cs.at[m, k], cr.at[m, zz], partner)

    def from_core(m, zz):
        return send(shard_of(m, zz, 1 - c), shard_of(m, zz, 1 - c), cs.at[m, 0], cr.at[m, zz], partner)

    def into(m):
        return pltpu.make_async_copy(own[m].at[number], vm[m], lin.at[m])

    def from_vm(m):
        return pltpu.make_async_copy(vm[m], shard_of(m, z, c), lout.at[m])

    order = range(len(others))
    for m in range(n):
        further(m, z, lambda copy: copy.start())
    for m in range(n):
        to_core(m, 3).start()
        into(m).start()
    for m in range(n):
        into(m).wait()
        from_vm(m).start()

    def pass_on(m):
        for k in order:
            from_z(m, others[k]).wait_recv()
            further(m, others[k], lambda copy: copy.start())
            to_x(m, k, others[k]).start()
            to_y(m, k, others[k]).start()

    def pass_across(m):
        for k in order:
            if (m + k) % 2:
                from_y(m, others[k]).wait_recv()
            else:
                from_x(m, others[k]).wait_recv()
            onward(m, k, others[k]).start()

    def finish(m):
        for k in order:
            if (m + k) % 2:
                from_x(m, others[k]).wait_recv()
            else:
                from_y(m, others[k]).wait_recv()
            from_onward(m, k, others[k]).wait_recv()
            to_core(m, k).start()

    for m in range(n + 2):
        if m < n:
            pass_on(m)
        if 0 <= m - 1 < n:
            pass_across(m - 1)
        if 0 <= m - 2 < n:
            finish(m - 2)
    for m in range(n):
        for o in others + [z]:
            from_core(m, o).wait_recv()
        for k in order:
            further(m, others[k], lambda copy: copy.wait_send())
            to_x(m, k, others[k]).wait_send()
            to_y(m, k, others[k]).wait_send()
            onward(m, k, others[k]).wait_send()
        further(m, z, lambda copy: copy.wait_send())
        for k in range(4):
            to_core(m, k).wait_send()
        from_vm(m).wait()


def gather(weights, number):
    n = len(weights)
    sems = [pltpu.SemaphoreType.DMA((n, 4))] * 11 + [pltpu.SemaphoreType.DMA((n,))] * 2
    return pl.pallas_call(
        functools.partial(_gather, n=n, number=number),
        in_specs=[pl.BlockSpec(memory_space=pltpu.HBM)] * n,
        out_specs=[pl.BlockSpec(memory_space=pltpu.HBM)] * n,
        out_shape=[_like(8 * w.shape[1], w.shape[2]) for w in weights],
        scratch_shapes=[pltpu.VMEM(w.shape[1:], bf16) for w in weights] + sems,
        compiler_params=pltpu.CompilerParams(collective_id=0, has_side_effects=True),
        name="gather",
    )(*weights)


def _reduce(g_ref, out_ref, own, got, low_in, high_in, low_out, high_out, sum_s, cs, cr, ls, lr, hs, hr, local, *, parts):
    rep, dp = lax.axis_index("rep"), lax.axis_index("dp")
    z, c = lax.div(dp, 2), lax.rem(dp, 2)
    chips, rows, wide = own.shape
    cols = wide // parts
    last = chips - 1
    partner = (rep, 2 * z + 1 - c)
    above, below = (rep, jnp.minimum(2 * z + 2, 2 * last) + c), (rep, jnp.maximum(2 * z - 2, 0) + c)
    barrier = pltpu.get_barrier_semaphore()
    peers = [partner] + [(rep, 2 * lax.rem(z + k, chips) + c) for k in range(1, chips)]
    for peer in peers:
        pl.semaphore_signal(barrier, inc=1, device_id=peer, device_id_type=MESH)
    pl.semaphore_wait(barrier, len(peers))

    def send(src, dst, send_sem, recv_sem, peer):
        return pltpu.make_async_remote_copy(src_ref=src, dst_ref=dst, send_sem=send_sem, recv_sem=recv_sem, device_id=peer, device_id_type=MESH)

    def block(chip, core):
        return g_ref.at[pl.ds(pl.multiple_of((2 * chip + core) * rows, rows), rows)]

    def across(chip):
        return send(block(chip, 1 - c), got.at[chip], cs.at[chip], cr.at[chip], partner)

    def kept(chip):
        return pltpu.make_async_copy(block(chip, c), own.at[chip], local.at[chip])

    def piece(ref, chip, p):
        return ref.at[chip, :, p * cols : (p + 1) * cols]

    def up(chip, p):
        return send(piece(low_out, chip, p), piece(low_in, chip, p), ls.at[chip, p], lr.at[chip, p], above)

    def down(chip, p):
        return send(piece(high_out, chip, p), piece(high_in, chip, p), hs.at[chip, p], hr.at[chip, p], below)

    def wide_of(ref, chip, p):
        return piece(ref, chip, p)[...].astype(f32)

    def mine(chip, p):
        return wide_of(own, chip, p) + wide_of(got, chip, p)

    def onward(chip, p, copy, came, leaves, first):
        @pl.when(first)
        def _():
            piece(leaves, chip, p)[...] = mine(chip, p).astype(bf16)

        @pl.when(jnp.logical_not(first))
        def _():
            copy(chip, p).wait_recv()
            piece(leaves, chip, p)[...] = (mine(chip, p) + wide_of(came, chip, p)).astype(bf16)

        copy(chip, p).start()

    for chip in range(chips):
        across(chip).start()
        kept(chip).start()
    for chip in range(chips):
        kept(chip).wait()
        across(chip).wait_recv()
    for k in range(last):
        for p in range(parts):

            @pl.when(z < last - k)
            def _(chip=last - k, p=p):
                onward(chip, p, up, low_in, low_out, z == 0)

            @pl.when(z > k)
            def _(chip=k, p=p):
                onward(chip, p, down, high_in, high_out, z == last)

    for p in range(parts):
        sum_s[...] = mine(z, p)

        @pl.when(z > 0)
        def _(p=p):
            up(z, p).wait_recv()
            sum_s[...] += wide_of(low_in, z, p)

        @pl.when(z < last)
        def _(p=p):
            down(z, p).wait_recv()
            sum_s[...] += wide_of(high_in, z, p)

        out_ref[:, p * cols : (p + 1) * cols] = sum_s[...].astype(bf16)

    for chip in range(chips):
        across(chip).wait_send()
    for k in range(last):
        for p in range(parts):

            @pl.when(z < last - k)
            def _(chip=last - k, p=p):
                up(chip, p).wait_send()

            @pl.when(z > k)
            def _(chip=k, p=p):
                down(chip, p).wait_send()


def reduce(g, parts):
    chips, rows, wide = 4, g.shape[0] // 8, g.shape[1]
    half = pltpu.VMEM((chips, rows, wide), bf16)
    sems = [pltpu.SemaphoreType.DMA((chips,))] * 2 + [pltpu.SemaphoreType.DMA((chips, parts))] * 4 + [pltpu.SemaphoreType.DMA((chips,))]
    return pl.pallas_call(
        functools.partial(_reduce, parts=parts), in_specs=[pl.BlockSpec(memory_space=pltpu.HBM)],
        out_specs=pl.BlockSpec(memory_space=pltpu.VMEM), out_shape=_like(rows, wide), scratch_shapes=[half] * 6 + [pltpu.VMEM((rows, wide // parts), f32)] + sems,
        compiler_params=pltpu.CompilerParams(collective_id=1, has_side_effects=True),
        cost_estimate=_estimate(rows * wide * 2**15, g), name="reduce",
    )(g)


NAMES = ("wq", "wk", "wv", "wo", "w_gate", "w_up", "w_down")


def solution(mesh):
    def fetched(weights, number):
        rep = lax.axis_index("rep")

        def gathered(*some):
            size = some[0].shape[1] // 4
            rows = [lax.dynamic_slice_in_dim(w[number], rep * size, size, 0) for w in some]
            return lax.all_gather(jnp.concatenate(rows, 1), ("dp", "rep"), axis=0, tiled=True)

        return gathered(weights[0]), gathered(*weights[1:3]), gathered(weights[3])

    def step(x, dy, *weights):
        layers = weights[0].shape[0]
        turn = table(x.shape[1])
        d = x.shape[2]
        some = [jnp.concatenate(weights[:4], 2), *weights[4:]]
        parts = lambda names, w: {name: (w, w.shape[1] // len(names), i) for i, name in enumerate(names)}
        gate, up = NAMES[4:6]
        got = gather(some, 0)
        whole = [parts(NAMES[:4], got[0]) | parts([gate], got[1]) | parts([up], got[2]) | parts(NAMES[6:], got[3])]
        for number in range(1, layers):
            got = fetched(some, number)
            whole.append(parts(NAMES[:4], got[0]) | parts([gate, up], got[1]) | parts(NAMES[6:], got[2]))
        h, kept = x[0], []
        for number, w in enumerate(whole):
            a, q, k, v = qkv(h, turn, w["wq"], w["wk"], w["wv"])
            o, lse = attend(q, k, v)
            kept.append([h, a, q, k, v, o, lse])
            last = number == layers - 1
            h1, b, gate, up, act, *h = ffn(h, o, w["wo"], w["w_gate"], w["w_up"], *([] if last else [w["w_down"]]))
            h = None if last else h[0]
            kept[-1] += [h1, b, gate, up, act]
        dh, mine = dy[0], [{} for _ in range(layers)]
        waiting = []

        def scatter(grad, like, room, put):
            grad, like = lax.optimization_barrier((grad, like))
            waiting.append([room, lax.psum_scatter(grad, "dp", scatter_dimension=0, tiled=True), put])
            return like

        def settled(like):
            for entry in waiting:
                entry[0] -= 1
            while waiting and waiting[0][0] <= 0:
                _, got, put = waiting.pop(0)
                like, got = lax.optimization_barrier((like, got))
                put(got)
            return like

        for number in reversed(range(layers)):
            w, out = whole[number], mine[number]
            h, a, q, k, v, o, lse, h1, b, gate, up, act = kept[number]

            def put(*names, out=out):
                return lambda got: out.update(zip(names, jnp.split(got, len(names), 1)))

            dh = scatter(by_weight(act, settled(dh), d, d), dh, 3, put(NAMES[-1]))
            dg, du, dh1, do, delta = ffn_back(h1, settled(dh), o, gate, up, w["wo"], w["w_gate"], w["w_up"], w["w_down"])
            do = scatter(by_ffn_weights(b, settled(dg), du), do, 6, put(*NAMES[4:6]))
            dq, dk, dv = attend_back(q, k, v, settled(do), lse, delta)
            dh, dqkv = qkv_back(h, dh1, settled(dq), dk, dv, turn, w["wq"], w["wk"], w["wv"])
            grad = by_attention_weights(a, settled(dqkv), o, dh1)
            if number:
                dh = scatter(grad, dh, 5, put(*NAMES[:4]))
            else:
                put(*NAMES[:4])(reduce(grad, 3))
        for _, got, put in waiting:
            put(got)
        return (dh[None], *(jnp.stack([got[name] for got in mine]) for name in NAMES))

    states, cut = P(("rep", "dp")), P(None, "dp")
    return jax.shard_map(
        step,
        mesh=mesh,
        in_specs=(states, states) + (cut,) * 7,
        out_specs=(states,) + (P("rep", "dp"),) * 7,
        check_vma=False,
    )
```
